32 devices in a mesh: blk: 8 (over z, y), layer: 4 (over x, core).
Axes of the slice: x: 2, y: 2, z: 4, core: 2. Of those that a mesh axis runs over, the one named last changes fastest.
Arguments:
- leaf_area: float32 [12, 16, 1024], P(None, 'layer', 'blk'), may hold values from 0 to 6
- soil_water: float32 [10, 1024], P(None, 'blk'), may hold values from 0.05 to 0.5
- root_share: float32 [16, 10], P('layer'), may hold values from 0 to 0.3
- patch_weight: float32 [16, 32768], P('layer', 'blk'), may hold values from 0 to 1
- patch_owner: int32 [32768, 1], P('blk'), may hold values from 0 to 7; in each aligned block of 4096 rows (0 to 4095, 4096 to 8191, ...) at most 1024 rows name the same one
- patch_local: int32 [32768], P('blk'), may hold values from 0 to 127
- month: int32 [1], replicated, may hold values from 0 to 11
- mix: float32 [1], replicated, may hold values from 0.1 to 0.9
Outputs:
- canopy_share: float32 [16, 1024], P('layer', 'blk')
The draws below stay inside these ranges and needn't reach their ends.
Inputs may be any that keep to these rules, and one draw needn't show every extreme that they name: `patch_owner`: among the rows of one device, no owner is named more than 1024 times, a bound that some block reaches.
All inputs are finite; a program needn't handle non-finite values.
Results may differ from the reference program's by a relative error of at most 0.000065.
Values sent between devices are 32-bit elements; how exact they have to be, the bound alone decides.
A program may use at most 64 MiB of HBM per device.

```python
import math
import jax
import jax.numpy as jnp
import numpy as np
from jax import lax

PFT = 16
MONTHS = 12
SOIL = 10
G_DEV = 128
P_DEV = 4096
GRID = 1024
PATCHES = 32768
CAP = 1024
N_BLK = 8


def touch_ends(drawn, rng, low, top_value):
    spot = [jax.random.randint(jax.random.fold_in(rng, axis), (), 0, length) for axis, length in enumerate(drawn.shape)]
    longest = drawn.shape.index(max(drawn.shape))
    next_to = spot[:longest] + [(spot[longest] + 1) % drawn.shape[longest]] + spot[longest + 1:]
    return drawn.at[tuple(spot)].set(low).at[tuple(next_to)].set(top_value)


def level_of(own_key, extent, pieces, low, top_value):
    def one(axis_at, parts):
        steps = jax.random.uniform(jax.random.fold_in(jax.random.fold_in(own_key, 6), axis_at), (parts,), jnp.float32, low / len(pieces), top_value / len(pieces))
        return jnp.repeat(jnp.exp(steps), extent[axis_at] // parts).reshape((-1,) + (1,) * (len(extent) - axis_at - 1))

    gain = one(*pieces[0])
    for cut in pieces[1:]:
        gain = gain * one(*cut)
    return gain


def assign_block(stream_key, own, number, rows, count, top, most, skew):
    ranking = jax.random.permutation(stream_key, count)
    heavy_load, usual = load_shares(count, rows * top, most, skew, True), load_shares(count, rows * top, most, skew, False)
    places = jnp.arange(count)

    def named(lengths, rotation):
        used = int((lengths > 0).sum())
        fixed = max(1, used // 4)
        passed = fixed + (places - fixed + rotation * (used - fixed)) % max(1, count - fixed)
        return jnp.zeros((count,), jnp.int32).at[ranking[jnp.where(places < fixed, places, passed)]].set(jnp.asarray(lengths, jnp.int32))

    lengths = jnp.where(number % 4 == 0, named(heavy_load, number // 4), named(usual, number - number // 4 - 1))
    mixed = jax.random.permutation(jax.random.fold_in(own, 3), count)
    source_of, receiver = mixed[0:count // 2 * 2:2], mixed[1:count // 2 * 2:2]
    margin = jnp.minimum(lengths[source_of] - 1, most - lengths[receiver]) // 2
    margin = jnp.where((source_of == ranking[0]) | (receiver == ranking[0]) | (lengths[receiver] == 0), 0, jnp.maximum(margin, 0))
    passed = jax.random.randint(jax.random.fold_in(own, 4), (count // 2,), 0, 1 << 20) % (margin + 1)
    lengths = lengths.at[source_of].add(-passed).at[receiver].add(passed)
    items = jnp.searchsorted(jnp.cumsum(lengths), jnp.arange(rows * top), side="right").astype(jnp.int32)
    table = items.reshape(top, rows).T
    table = table[jax.random.permutation(jax.random.fold_in(own, 1), rows)]
    rotation = jax.random.randint(jax.random.fold_in(own, 2), (rows, 1), 0, top)
    return jnp.take_along_axis(table, (jnp.arange(top)[None, :] + rotation) % top, axis=1)


def load_shares(count, total, reach, skew, full):
    weights = [(1 << 20) // math.isqrt(standing ** skew) + 1 for standing in range(1, count + 1)]
    largest = reach if full else min(reach, max(-(-total // count), total * weights[0] // sum(weights)))
    least = 1 if total - largest >= count - 1 else 0
    counts, surplus = [largest] + [least] * (count - 1), total - largest - least * (count - 1)
    while surplus > 0:
        free = [i for i in range(1, count) if counts[i] < largest] or [i for i in range(1, count) if counts[i] < reach]
        mass, left = sum([weights[i] for i in free]), surplus
        for i in free:
            addition = min(reach - counts[i], max(1, left * weights[i] // mass), surplus)
            counts[i] = counts[i] + addition
            surplus = surplus - addition
    return np.array(counts)


def setup_inputs(seed: int = 0) -> dict:
    keys = jax.random.split(jax.random.key(seed), 9)
    leaf_area = jnp.clip(6.0 * jax.random.uniform(keys[0], (MONTHS, PFT, GRID), jnp.float32) ** level_of(keys[0], (MONTHS, PFT, GRID), ((1, 4), (2, 8)), -0.2, 0.2), 0.0, 6.0)
    soil_water = jnp.clip(0.05 + 0.45 * jax.random.uniform(keys[1], (SOIL, GRID), jnp.float32) ** level_of(keys[1], (SOIL, GRID), ((1, 8),), -0.2, 0.2), 0.05, 0.5)
    root_share = jnp.clip(0.3 * jax.random.uniform(keys[2], (PFT, SOIL), jnp.float32) ** level_of(keys[2], (PFT, SOIL), ((0, 4),), -0.2, 0.2), 0.0, 0.3)
    patch_weight = jnp.clip(1.0 * jax.random.uniform(keys[3], (PFT, PATCHES), jnp.float32) ** level_of(keys[3], (PFT, PATCHES), ((0, 4), (1, 8)), -0.2, 0.2), 0.0, 1.0)
    patch_owner_keys = jax.random.split(jax.random.fold_in(keys[4], 1), PATCHES // P_DEV)
    patch_owner_turns = jax.random.permutation(jax.random.fold_in(keys[4], 3), PATCHES // P_DEV)
    patch_owner = jax.vmap(lambda own, number: assign_block(jax.random.fold_in(keys[4], 2), own, number, P_DEV, N_BLK, 1, CAP, 2))(patch_owner_keys, patch_owner_turns).reshape((PATCHES, 1))
    patch_local = touch_ends(jax.random.randint(keys[5], (PATCHES,), 0, G_DEV), jax.random.fold_in(keys[5], 1), 0, G_DEV - 1).astype(jnp.int32)
    month = jax.random.randint(keys[6], (1,), 0, MONTHS).astype(jnp.int32)
    mix = jnp.clip(jax.random.uniform(keys[7], (1,), jnp.float32, 0.1, 0.9), 0.1, 0.9)
    return dict(leaf_area=leaf_area, soil_water=soil_water, root_share=root_share, patch_weight=patch_weight, patch_owner=patch_owner, patch_local=patch_local, month=month, mix=mix)


def interpolate(leaf_area, month, mix):
    earlier_index = month[0]
    second = (earlier_index + 1) % MONTHS
    earlier = lax.dynamic_index_in_dim(leaf_area, earlier_index, 0, keepdims=False)
    later = lax.dynamic_index_in_dim(leaf_area, second, 0, keepdims=False)
    return mix[0] * earlier + (1.0 - mix[0]) * later


def reference(leaf_area, soil_water, root_share, patch_weight, patch_owner, patch_local, month, mix):
    patch_cell = (patch_owner[:, 0] * G_DEV + patch_local).astype(jnp.int32)
    current = interpolate(leaf_area, month, mix)
    patch_leaf = jnp.take(current, patch_cell, axis=1)
    patch_soil = jnp.take(soil_water, patch_cell, axis=1)
    stress = jnp.dot(root_share, patch_soil, precision=lax.Precision.HIGHEST)
    canopy = patch_weight * (1.0 - jnp.exp(-0.5 * patch_leaf)) * stress
    grid_sum = jax.ops.segment_sum(canopy.T, patch_cell, num_segments=GRID).T
    total = jnp.sum(grid_sum, axis=0)
    return grid_sum / (1.0 + total)
```

```python
import functools

import jax
import jax.numpy as jnp
from jax import lax
from jax.experimental import pallas as pl
from jax.experimental.pallas import tpu as pltpu
from jax.sharding import PartitionSpec as P

MESH = pl.DeviceIdType.MESH
CHUNK = 512


def local_sums(weight, owner, local, owners, cells):
    types, patches = weight.shape
    chunk = CHUNK if patches % CHUNK == 0 else patches
    row_owner = lax.broadcasted_iota(jnp.int32, (owners * types, chunk), 0) // types
    cell = lax.broadcasted_iota(jnp.int32, (cells, chunk), 0)
    total = None
    for start in range(0, patches, chunk):
        part = slice(start, start + chunk)
        w = weight[:, part]
        high = w.astype(jnp.bfloat16).astype(jnp.float32)
        low = w - high
        named = row_owner == owner[:, part]
        left = jnp.concatenate(
            [
                jnp.where(named, jnp.concatenate([piece] * owners, axis=0), 0.0)
                for piece in (high, low)
            ],
            axis=0,
        ).astype(jnp.bfloat16)
        table = jnp.where(cell == local[:, part], 1.0, 0.0).astype(jnp.bfloat16)
        product = lax.dot_general(
            left, table, (((1,), (1,)), ((), ())), preferred_element_type=jnp.float32
        )
        total = product if total is None else total + product
    return total[: owners * types] + total[owners * types :]


def kernel(
    n, m, leaf_hbm, soil_hbm, root_hbm, weight_hbm, owner_hbm, local_hbm, month_hbm, mix_hbm,
    out_ref, leaf, soil, root, weight, owner, local, month, mix,
    sums, pair, got_sums, got_pairs, load_sem, send_sem, recv_sem,
):
    blk, layer = lax.axis_index("blk"), lax.axis_index("layer")
    types, cells = out_ref.shape
    loads = [
        pltpu.make_async_copy(source, target, load_sem.at[i])
        for i, (source, target) in enumerate(
            (
                (weight_hbm, weight),
                (owner_hbm, owner),
                (local_hbm, local),
                (month_hbm, month),
                (mix_hbm, mix),
                (leaf_hbm, leaf),
                (soil_hbm, soil),
                (root_hbm, root),
            )
        )
    ]
    for load in loads:
        load.start()

    def device(step_blk, step_layer):
        return (lax.rem(blk + step_blk, n), lax.rem(layer + step_layer, m))

    steps = [(i, j) for i in range(n) for j in range(m) if i or j]
    barrier = pltpu.get_barrier_semaphore()
    for step in steps:
        pl.semaphore_signal(barrier, inc=1, device_id=device(*step), device_id_type=MESH)

    for load in loads[:3]:
        load.wait()
    partial = local_sums(weight, owner, local, n, cells)
    for i in range(n):
        sums[i] = partial[i * types : (i + 1) * types]
    for load in loads[3:]:
        load.wait()
    first = month[0]
    second = lax.rem(first + 1, leaf.shape[0])
    current = mix[0] * leaf[first] + (1.0 - mix[0]) * leaf[second]
    stress = root[:, 0:1] * soil[0:1, :]
    for i in range(1, soil.shape[0]):
        stress += root[:, i : i + 1] * soil[i : i + 1, :]
    effect = (1.0 - jnp.exp(-0.5 * current)) * stress
    own = sums[blk]
    pair[0] = own
    pair[1] = effect

    pl.semaphore_wait(barrier, len(steps))
    for i, j in reversed(steps):
        if i:
            source, target, k = (
                sums.at[lax.rem(blk + i, n)],
                got_sums.at[j * (n - 1) + i - 1],
                0,
            )
        else:
            source, target, k = pair, got_pairs.at[j - 1], 1
        pltpu.make_async_remote_copy(
            src_ref=source,
            dst_ref=target,
            send_sem=send_sem.at[k],
            recv_sem=recv_sem.at[k],
            device_id=device(i, j),
            device_id_type=MESH,
        ).start()
    pltpu.make_async_copy(got_sums, got_sums, recv_sem.at[0]).wait()
    pltpu.make_async_copy(got_pairs, got_pairs, recv_sem.at[1]).wait()

    mine, everyone = None, None
    for j in range(m):
        grid = own if j == 0 else got_pairs[j - 1, 0]
        for i in range(n - 1):
            grid = grid + got_sums[j * (n - 1) + i]
        grid = grid * (effect if j == 0 else got_pairs[j - 1, 1])
        if j == 0:
            mine = grid
            everyone = grid
        else:
            everyone = everyone + grid
    out_ref[...] = mine / (1.0 + jnp.sum(everyone, axis=0, keepdims=True))
    pltpu.make_async_copy(got_sums, got_sums, send_sem.at[0]).wait()
    pltpu.make_async_copy(got_pairs, got_pairs, send_sem.at[1]).wait()


def on_device(
    leaf_area, soil_water, root_share, patch_weight, patch_owner, patch_local, month, mix
):
    n, m = lax.axis_size("blk"), lax.axis_size("layer")
    months, types, cells = leaf_area.shape
    patches = patch_local.shape[0]
    owner = patch_owner.reshape(1, patches)
    local = patch_local.reshape(1, patches)
    f32, i32 = jnp.float32, jnp.int32
    return pl.pallas_call(
        functools.partial(kernel, n, m),
        out_shape=jax.ShapeDtypeStruct((types, cells), f32),
        in_specs=[pl.BlockSpec(memory_space=pl.ANY)] * 8,
        out_specs=pl.BlockSpec(memory_space=pltpu.VMEM),
        scratch_shapes=[
            pltpu.VMEM(leaf_area.shape, f32),
            pltpu.VMEM(soil_water.shape, f32),
            pltpu.VMEM(root_share.shape, f32),
            pltpu.VMEM(patch_weight.shape, f32),
            pltpu.VMEM(owner.shape, i32),
            pltpu.VMEM(local.shape, i32),
            pltpu.SMEM(month.shape, i32),
            pltpu.SMEM(mix.shape, f32),
            pltpu.VMEM((n, types, cells), f32),
            pltpu.VMEM((2, types, cells), f32),
            pltpu.VMEM((m * (n - 1), types, cells), f32),
            pltpu.VMEM((m - 1, 2, types, cells), f32),
            pltpu.SemaphoreType.DMA((8,)),
            pltpu.SemaphoreType.DMA((2,)),
            pltpu.SemaphoreType.DMA((2,)),
        ],
        compiler_params=pltpu.CompilerParams(collective_id=0, has_side_effects=True),
    )(leaf_area, soil_water, root_share, patch_weight, owner, local, month, mix)


def solution(mesh):
    in_specs = (
        P(None, "layer", "blk"),
        P(None, "blk"),
        P("layer", None),
        P("layer", "blk"),
        P("blk", None),
        P("blk"),
        P(),
        P(),
    )
    out_specs = P("layer", "blk")
    return jax.shard_map(
        on_device, mesh=mesh, in_specs=in_specs, out_specs=out_specs, check_vma=False
    )
```

```python
import functools

import jax
import jax.numpy as jnp
from jax import lax
from jax.experimental import pallas as pl
from jax.experimental.pallas import tpu as pltpu
from jax.sharding import PartitionSpec as P

MESH = pl.DeviceIdType.MESH
CHUNK = 512


def local_sums(weight, owner, local, owners, cells):
    types, patches = weight.shape
    chunk = CHUNK if patches % CHUNK == 0 else patches
    row_owner = lax.broadcasted_iota(jnp.int32, (owners * types, chunk), 0) // types
    cell = lax.broadcasted_iota(jnp.int32, (cells, chunk), 0)
    total = None
    for start in range(0, patches, chunk):
        part = slice(start, start + chunk)
        w = weight[:, part]
        high = w.astype(jnp.bfloat16).astype(jnp.float32)
        low = w - high
        named = row_owner == owner[:, part]
        left = jnp.concatenate(
            [
                jnp.where(named, jnp.concatenate([piece] * owners, axis=0), 0.0)
                for piece in (high, low)
            ],
            axis=0,
        ).astype(jnp.bfloat16)
        table = jnp.where(cell == local[:, part], 1.0, 0.0).astype(jnp.bfloat16)
        product = lax.dot_general(
            left, table, (((1,), (1,)), ((), ())), preferred_element_type=jnp.float32
        )
        total = product if total is None else total + product
    return total[: owners * types] + total[owners * types :]


def kernel(
    n, m, leaf_hbm, soil_hbm, root_hbm, weight_hbm, owner_hbm, local_hbm, month_hbm, mix_hbm,
    out_ref, leaf, soil, root, weight, owner, local, month, mix,
    sums, pair, got_sums, got_pairs, load_sem, send_sem, recv_sem,
):
    blk, layer = lax.axis_index("blk"), lax.axis_index("layer")
    types, cells = out_ref.shape
    loads = [
        pltpu.make_async_copy(source, target, load_sem.at[i])
        for i, (source, target) in enumerate(
            (
                (weight_hbm, weight),
                (owner_hbm, owner),
                (local_hbm, local),
                (month_hbm, month),
                (mix_hbm, mix),
                (leaf_hbm, leaf),
                (soil_hbm, soil),
                (root_hbm, root),
            )
        )
    ]
    for load in loads:
        load.start()

    def device(step_blk, step_layer):
        return (lax.rem(blk + step_blk, n), lax.rem(layer + step_layer, m))

    steps = [(i, j) for i in range(n) for j in range(m) if i or j]
    barrier = pltpu.get_barrier_semaphore()
    for step in steps:
        pl.semaphore_signal(barrier, inc=1, device_id=device(*step), device_id_type=MESH)

    for load in loads[:3]:
        load.wait()
    partial = local_sums(weight, owner, local, n, cells)
    for i in range(n):
        sums[i] = partial[i * types : (i + 1) * types]
    for load in loads[3:]:
        load.wait()
    first = month[0]
    second = lax.rem(first + 1, leaf.shape[0])
    current = mix[0] * leaf[first] + (1.0 - mix[0]) * leaf[second]
    stress = root[:, 0:1] * soil[0:1, :]
    for i in range(1, soil.shape[0]):
        stress += root[:, i : i + 1] * soil[i : i + 1, :]
    effect = (1.0 - jnp.exp(-0.5 * current)) * stress
    own = sums[blk]
    pair[0] = own
    pair[1] = effect

    pl.semaphore_wait(barrier, len(steps))
    for i, j in reversed(steps):
        if i:
            source, target, k = (
                sums.at[lax.rem(blk + i, n)],
                got_sums.at[j * (n - 1) + i - 1],
                0,
            )
        else:
            source, target, k = pair, got_pairs.at[j - 1], 1
        pltpu.make_async_remote_copy(
            src_ref=source,
            dst_ref=target,
            send_sem=send_sem.at[k],
            recv_sem=recv_sem.at[k],
            device_id=device(i, j),
            device_id_type=MESH,
        ).start()
    pltpu.make_async_copy(got_sums, got_sums, recv_sem.at[0]).wait()
    pltpu.make_async_copy(got_pairs, got_pairs, recv_sem.at[1]).wait()

    mine, everyone = None, None
    for j in range(m):
        grid = own if j == 0 else got_pairs[j - 1, 0]
        for i in range(n - 1):
            grid = grid + got_sums[j * (n - 1) + i]
        grid = grid * (effect if j == 0 else got_pairs[j - 1, 1])
        if j == 0:
            mine = grid
            everyone = grid
        else:
            everyone = everyone + grid
    out_ref[...] = mine / (1.0 + jnp.sum(everyone, axis=0, keepdims=True))
    pltpu.make_async_copy(got_sums, got_sums, send_sem.at[0]).wait()
    pltpu.make_async_copy(got_pairs, got_pairs, send_sem.at[1]).wait()


def on_device(
    leaf_area, soil_water, root_share, patch_weight, patch_owner, patch_local, month, mix
):
    n, m = lax.axis_size("blk"), lax.axis_size("layer")
    months, types, cells = leaf_area.shape
    patches = patch_local.shape[0]
    owner = patch_owner.reshape(1, patches)
    local = patch_local.reshape(1, patches)
    f32, i32 = jnp.float32, jnp.int32
    return pl.pallas_call(
        functools.partial(kernel, n, m),
        out_shape=pltpu.VMEM((types, cells), f32),
        in_specs=[pl.BlockSpec(memory_space=pl.ANY)] * 8,
        out_specs=pl.BlockSpec(memory_space=pltpu.VMEM),
        scratch_shapes=[
            pltpu.VMEM(leaf_area.shape, f32),
            pltpu.VMEM(soil_water.shape, f32),
            pltpu.VMEM(root_share.shape, f32),
            pltpu.VMEM(patch_weight.shape, f32),
            pltpu.VMEM(owner.shape, i32),
            pltpu.VMEM(local.shape, i32),
            pltpu.SMEM(month.shape, i32),
            pltpu.SMEM(mix.shape, f32),
            pltpu.VMEM((n, types, cells), f32),
            pltpu.VMEM((2, types, cells), f32),
            pltpu.VMEM((m * (n - 1), types, cells), f32),
            pltpu.VMEM((m - 1, 2, types, cells), f32),
            pltpu.SemaphoreType.DMA((8,)),
            pltpu.SemaphoreType.DMA((2,)),
            pltpu.SemaphoreType.DMA((2,)),
        ],
        compiler_params=pltpu.CompilerParams(collective_id=0, has_side_effects=True),
    )(leaf_area, soil_water, root_share, patch_weight, owner, local, month, mix)


def solution(mesh):
    in_specs = (
        P(None, "layer", "blk"),
        P(None, "blk"),
        P("layer", None),
        P("layer", "blk"),
        P("blk", None),
        P("blk"),
        P(),
        P(),
    )
    out_specs = P("layer", "blk")
    return jax.shard_map(
        on_device, mesh=mesh, in_specs=in_specs, out_specs=out_specs, check_vma=False
    )
```

```python
import functools

import jax
import jax.numpy as jnp
from jax import lax
from jax.experimental import pallas as pl
from jax.experimental.pallas import tpu as pltpu
from jax.sharding import PartitionSpec as P

MESH = pl.DeviceIdType.MESH
CHUNK = 512


def local_sums(weight, owner, local, owners, cells):
    types, patches = weight.shape
    chunk = CHUNK if patches % CHUNK == 0 else patches
    row_owner = lax.broadcasted_iota(jnp.int32, (owners * types, chunk), 0) // types
    cell = lax.broadcasted_iota(jnp.int32, (cells, chunk), 0)
    total = None
    for start in range(0, patches, chunk):
        part = slice(start, start + chunk)
        w = weight[:, part]
        high = w.astype(jnp.bfloat16).astype(jnp.float32)
        low = w - high
        named = row_owner == owner[:, part]
        left = jnp.concatenate(
            [
                jnp.where(named, jnp.concatenate([piece] * owners, axis=0), 0.0)
                for piece in (high, low)
            ],
            axis=0,
        ).astype(jnp.bfloat16)
        table = jnp.where(cell == local[:, part], 1.0, 0.0).astype(jnp.bfloat16)
        product = lax.dot_general(
            left, table, (((1,), (1,)), ((), ())), preferred_element_type=jnp.float32
        )
        total = product if total is None else total + product
    return total[: owners * types] + total[owners * types :]


def kernel(
    n, m, leaf_hbm, soil_hbm, root_hbm, weight_hbm, owner_hbm, local_hbm, month_hbm, mix_hbm,
    out_ref, leaf, soil, root, weight, owner, local, month, mix,
    sums, pair, got_sums, got_pairs, load_sem, send_sem, recv_sem,
):
    blk, layer = lax.axis_index("blk"), lax.axis_index("layer")
    types, cells = out_ref.shape
    loads = [
        pltpu.make_async_copy(source, target, load_sem.at[i])
        for i, (source, target) in enumerate(
            (
                (weight_hbm, weight),
                (owner_hbm, owner),
                (local_hbm, local),
                (month_hbm, month),
                (mix_hbm, mix),
                (leaf_hbm, leaf),
                (soil_hbm, soil),
                (root_hbm, root),
            )
        )
    ]
    for load in loads:
        load.start()

    def device(step_blk, step_layer):
        return (lax.rem(blk + step_blk, n), lax.rem(layer + step_layer, m))

    steps = [(i, j) for i in range(n) for j in range(m) if i or j]
    barrier = pltpu.get_barrier_semaphore()
    for step in steps:
        pl.semaphore_signal(barrier, inc=1, device_id=device(*step), device_id_type=MESH)

    for load in loads[:3]:
        load.wait()
    partial = local_sums(weight, owner, local, n, cells)
    for i in range(n):
        sums[i] = partial[i * types : (i + 1) * types]
    for load in loads[3:]:
        load.wait()
    first = month[0]
    second = lax.rem(first + 1, leaf.shape[0])
    current = mix[0] * leaf[first] + (1.0 - mix[0]) * leaf[second]
    stress = root[:, 0:1] * soil[0:1, :]
    for i in range(1, soil.shape[0]):
        stress += root[:, i : i + 1] * soil[i : i + 1, :]
    effect = (1.0 - jnp.exp(-0.5 * current)) * stress
    own = sums[blk]
    pair[0] = own
    pair[1] = effect

    pl.semaphore_wait(barrier, len(steps))
    for i, j in steps:
        if i:
            source, target, k = (
                sums.at[lax.rem(blk + i, n)],
                got_sums.at[j * (n - 1) + i - 1],
                0,
            )
        else:
            source, target, k = pair, got_pairs.at[j - 1], 1
        pltpu.make_async_remote_copy(
            src_ref=source,
            dst_ref=target,
            send_sem=send_sem.at[k],
            recv_sem=recv_sem.at[k],
            device_id=device(i, j),
            device_id_type=MESH,
        ).start()
    pltpu.make_async_copy(got_sums, got_sums, recv_sem.at[0]).wait()
    pltpu.make_async_copy(got_pairs, got_pairs, recv_sem.at[1]).wait()

    mine, everyone = None, None
    for j in range(m):
        grid = own if j == 0 else got_pairs[j - 1, 0]
        for i in range(n - 1):
            grid = grid + got_sums[j * (n - 1) + i]
        grid = grid * (effect if j == 0 else got_pairs[j - 1, 1])
        if j == 0:
            mine = grid
            everyone = grid
        else:
            everyone = everyone + grid
    out_ref[...] = mine / (1.0 + jnp.sum(everyone, axis=0, keepdims=True))
    pltpu.make_async_copy(got_sums, got_sums, send_sem.at[0]).wait()
    pltpu.make_async_copy(got_pairs, got_pairs, send_sem.at[1]).wait()


def on_device(
    leaf_area, soil_water, root_share, patch_weight, patch_owner, patch_local, month, mix
):
    n, m = lax.axis_size("blk"), lax.axis_size("layer")
    months, types, cells = leaf_area.shape
    patches = patch_local.shape[0]
    owner = patch_owner.reshape(1, patches)
    local = patch_local.reshape(1, patches)
    f32, i32 = jnp.float32, jnp.int32
    return pl.pallas_call(
        functools.partial(kernel, n, m),
        out_shape=pltpu.VMEM((types, cells), f32),
        in_specs=[pl.BlockSpec(memory_space=pl.ANY)] * 8,
        out_specs=pl.BlockSpec(memory_space=pltpu.VMEM),
        scratch_shapes=[
            pltpu.VMEM(leaf_area.shape, f32),
            pltpu.VMEM(soil_water.shape, f32),
            pltpu.VMEM(root_share.shape, f32),
            pltpu.VMEM(patch_weight.shape, f32),
            pltpu.VMEM(owner.shape, i32),
            pltpu.VMEM(local.shape, i32),
            pltpu.SMEM(month.shape, i32),
            pltpu.SMEM(mix.shape, f32),
            pltpu.VMEM((n, types, cells), f32),
            pltpu.VMEM((2, types, cells), f32),
            pltpu.VMEM((m * (n - 1), types, cells), f32),
            pltpu.VMEM((m - 1, 2, types, cells), f32),
            pltpu.SemaphoreType.DMA((8,)),
            pltpu.SemaphoreType.DMA((2,)),
            pltpu.SemaphoreType.DMA((2,)),
        ],
        compiler_params=pltpu.CompilerParams(collective_id=0, has_side_effects=True),
    )(leaf_area, soil_water, root_share, patch_weight, owner, local, month, mix)


def solution(mesh):
    in_specs = (
        P(None, "layer", "blk"),
        P(None, "blk"),
        P("layer", None),
        P("layer", "blk"),
        P("blk", None),
        P("blk"),
        P(),
        P(),
    )
    out_specs = P("layer", "blk")
    return jax.shard_map(
        on_device, mesh=mesh, in_specs=in_specs, out_specs=out_specs, check_vma=False
    )
```
